32 devices in a mesh: ep: 4 (over y, x), tp: 4 (over z), dp: 2 (over core).
Axes of the slice: x: 2, y: 2, z: 4, core: 2. Of those that a mesh axis runs over, the one named last changes fastest.
Arguments:
- down_weight: bfloat16 [4, 16384, 3072], P('ep', 'tp', 'dp'), may hold values from -130 to 130
- owned_span: int32 [4, 4, 2], replicated, may hold values from 0 to 31, as said below
Outputs:
- saved_spans: bfloat16 [4, 4, 768, 16384], P('ep', 'tp', 'dp')
The draws below stay inside these ranges and needn't reach their ends.
Inputs may be any that keep to these rules, and one draw needn't show every extreme that they name: `owned_span`: block g holds rows (g % 8) * 384 onward of expert g // 8; every block is stored by exactly one device; the block at [i, j, k] has (g % 8) // 4 == k; for each k the experts of the stored blocks form a Latin square over i and j: each expert once for each i and once for each j.
All inputs are finite; a program needn't handle non-finite values.
Results may differ from the reference program's by a relative error of at most 0.001.
Values may be sent and summed in bfloat16 or wider, within the bound.
A program may use at most 128 MiB of HBM per device.

```python
import jax
import jax.numpy as jnp

FF = 16384
EXPERTS = 4
SLAB = 3072
BLOCK_ROWS = 384
N_EP = 4
N_TP = 4
N_DP = 2


def permuted_rows(key, count_rows, width):
    scores = jax.random.randint(key, (count_rows, width), 0, 1 << 20) * width + jnp.arange(width, dtype=jnp.int32)[None, :]
    return jnp.argsort(scores, axis=1).astype(jnp.int32)


def draw_owned_span(key, part):
    key_list = jax.random.split(jax.random.fold_in(key, 23), 4)
    per_expert = N_TP * N_DP
    row_perm = permuted_rows(key_list[0], N_DP, N_EP)
    col_perm = permuted_rows(key_list[1], N_DP, N_TP)
    relabel = permuted_rows(key_list[2], N_DP, N_EP)
    block_perm = permuted_rows(key_list[3], N_DP * N_EP, N_TP).reshape(N_DP, N_EP, N_TP)
    summed = (row_perm[:, :, None] + col_perm[:, None, :]) % N_EP
    latin_square = jnp.take_along_axis(relabel[:, :, None], summed.reshape(N_DP, N_EP * N_TP, 1), axis=1).reshape(N_DP, N_EP, N_TP)
    replica_ids = jnp.arange(N_DP, dtype=jnp.int32)[:, None, None] + jnp.zeros((N_DP, N_EP, N_TP), jnp.int32)
    ep_ids = jnp.arange(N_EP, dtype=jnp.int32)[None, :, None] + jnp.zeros((N_DP, N_EP, N_TP), jnp.int32)
    within = replica_ids * N_TP + block_perm[replica_ids, latin_square, ep_ids]
    global_ids = latin_square * per_expert + within
    return jnp.transpose(global_ids, (1, 2, 0)).astype(jnp.int32)


def draw_down_weight(key, part):
    key_list = jax.random.split(jax.random.fold_in(key, 11), 3)
    base_draw = jnp.clip(jax.random.normal(key_list[0], (EXPERTS, FF, SLAB), jnp.float32), -4.0, 4.0)
    spread = 1.15
    row_scale = jnp.exp(jax.random.uniform(key_list[1], (SLAB,), jnp.float32, -spread, spread))
    col_scale = jnp.exp(jax.random.uniform(key_list[2], (FF,), jnp.float32, -spread, spread))
    expert_scale = jnp.power(3.0, jnp.arange(EXPERTS, dtype=jnp.float32) / max(EXPERTS - 1, 1))
    values = base_draw * expert_scale[:, None, None] * col_scale[None, :, None] * row_scale[None, None, :]
    return values.astype(jnp.bfloat16)


def setup_inputs(seed: int = 0) -> dict:
    keys = jax.random.split(jax.random.key(seed), 3)
    down_weight = draw_down_weight(jax.random.fold_in(keys[2], 71), 0)
    owned_span = draw_owned_span(jax.random.fold_in(keys[2], 71), 0)
    return {"down_weight": down_weight, "owned_span": owned_span}


def reference(down_weight, owned_span):
    per_expert = N_TP * N_DP
    saved_rows = jnp.transpose(down_weight, (0, 2, 1)).reshape(EXPERTS * per_expert, BLOCK_ROWS, FF)
    owner_list = owned_span.reshape(-1).astype(jnp.int32)
    picked = jnp.take(saved_rows, owner_list, axis=0)
    saved_spans = picked.reshape(N_EP, N_TP, N_DP * BLOCK_ROWS, FF)
    return saved_spans
```

```python
import functools

import jax
import jax.numpy as jnp
from jax import lax
from jax.experimental import pallas as pl
from jax.experimental.pallas import tpu as pltpu
from jax.sharding import PartitionSpec as P

MESH = pl.DeviceIdType.MESH
LANES = 128
SUBLANES = 16
CHUNK = 256
STAGES = 4
AHEAD = 2
SPARE = 3 << 20
WRITES = 8


def pick(values, index):
    chosen = values[0]
    for b in range(1, len(values)):
        chosen = jnp.where(index == b, values[b], chosen)
    return chosen


def kernel(n_ep, n_tp, n_dp, chunk, weight, span, out, stage, turned, send, relay,
           load_sem, ep_send, ep_recv, tp_send, tp_recv, own_sem, *arrived):
    my_ep = lax.axis_index("ep")
    my_tp = lax.axis_index("tp")
    my_dp = lax.axis_index("dp")
    hidden, width = weight.shape[1], weight.shape[2]
    rows = width // n_tp
    chunks = hidden // chunk
    per_expert = n_tp * n_dp

    def load(c):
        return pltpu.make_async_copy(
            weight.at[0, pl.ds(c * chunk, chunk)], stage.at[c % STAGES], load_sem.at[c % STAGES])

    def to_ep(c, d):
        return pltpu.make_async_remote_copy(
            send.at[c, d], arrived[c].at[d], ep_send.at[c, d], ep_recv.at[c, d],
            device_id={"ep": lax.rem(my_ep + d, n_ep)}, device_id_type=MESH)

    def columns(tp, c):
        return out.at[0, 0, :, pl.ds(pl.multiple_of(tp * hidden + c * chunk, chunk), chunk)]

    def to_tp(c, d):
        return pltpu.make_async_remote_copy(
            relay.at[c, d], columns(my_tp, c), tp_send.at[c, d], tp_recv.at[c, d],
            device_id={"tp": lax.rem(my_tp + d, n_tp)}, device_id_type=MESH)

    def from_tp(c, d):
        return pltpu.make_async_remote_copy(
            relay.at[c, d], columns(lax.rem(my_tp + n_tp - d, n_tp), c), tp_send.at[c, d], tp_recv.at[c, d],
            device_id={"tp": lax.rem(my_tp + d, n_tp)}, device_id_type=MESH)

    def own(c):
        return pltpu.make_async_copy(relay.at[c, 0], columns(my_tp, c), own_sem.at[c])

    for c in range(min(STAGES, chunks)):
        load(c).start()

    barrier = pltpu.get_barrier_semaphore()
    for d in range(1, n_ep):
        pl.semaphore_signal(barrier, inc=1, device_id={"ep": lax.rem(my_ep + d, n_ep)}, device_id_type=MESH)
    for d in range(1, n_tp):
        pl.semaphore_signal(barrier, inc=1, device_id={"tp": lax.rem(my_tp + d, n_tp)}, device_id_type=MESH)

    wanted = []
    for d in range(n_ep):
        i = lax.rem(my_ep + d, n_ep)
        total = jnp.int32(0)
        for j in range(n_tp):
            g = span[i, my_dp, j]
            total = total + jnp.where(g // per_expert == my_ep, g % per_expert - my_dp * n_tp, 0)
        wanted.append(total)
    slot = []
    for d in range(n_tp):
        j = lax.rem(my_tp + d, n_tp)
        slot.append(lax.rem(my_ep + n_ep - span[my_ep, my_dp, j] // per_expert, n_ep))

    def first_half(c):
        load(c).wait()

        @pl.loop(0, width // LANES)
        def _(b):
            at = pl.multiple_of(b * LANES, LANES)
            turned[pl.ds(at, LANES), :] = stage[c % STAGES, :, pl.ds(at, LANES)].T

        if c == 0:
            pl.semaphore_wait(barrier, n_ep + n_tp - 2)
        if c + STAGES < chunks:
            load(c + STAGES).start()
        for d in range(n_ep - 1, -1, -1):
            block = pick([turned[b * rows:(b + 1) * rows, :] for b in range(n_tp)], wanted[d])
            if d == 0:
                arrived[c][0] = block
            else:
                send[c, d] = block
                to_ep(c, d).start()

    def second_half(c):
        for d in range(1, n_ep):
            to_ep(c, d).wait_recv()
        for d in range(n_tp - 1, -1, -1):
            relay[c, d] = pick([arrived[c][s] for s in range(n_ep)], slot[d])
            if d == 0:
                own(c).start()
            else:
                to_tp(c, d).start()

    for step in range(chunks + AHEAD):
        if step < chunks:
            first_half(step)
        if step >= AHEAD:
            second_half(step - AHEAD)

    for c in range(chunks):
        for d in range(1, n_ep):
            to_ep(c, d).wait_send()
        for d in range(1, n_tp):
            from_tp(c, d).wait_recv()
            to_tp(c, d).wait_send()
        own(c).wait()


def writer(saved, out, sem):
    pieces = sem.shape[0]
    rows = saved.shape[2] // pieces
    copies = [
        pltpu.make_async_copy(
            saved.at[0, 0, pl.ds(p * rows, rows)], out.at[0, 0, pl.ds(p * rows, rows)], sem.at[p])
        for p in range(pieces)
    ]
    for copy in copies:
        copy.start()
    for copy in copies:
        copy.wait()


def write_out(saved):
    tiles = max(saved.shape[2] // SUBLANES, 1)
    pieces = max(p for p in range(1, WRITES + 1) if tiles % p == 0)
    return pl.pallas_call(
        writer,
        out_shape=jax.ShapeDtypeStruct(saved.shape, saved.dtype),
        in_specs=[pl.BlockSpec(memory_space=pltpu.VMEM)],
        out_specs=pl.BlockSpec(memory_space=pl.ANY),
        scratch_shapes=[pltpu.SemaphoreType.DMA((pieces,))],
        compiler_params=pltpu.CompilerParams(vmem_limit_bytes=SPARE),
    )(saved)


def local(down_weight, owned_span):
    n_ep, n_tp, n_dp = (lax.axis_size(a) for a in ("ep", "tp", "dp"))
    _, hidden, width = down_weight.shape
    rows = width // n_tp
    chunk = min(CHUNK, hidden)
    chunks = hidden // chunk
    kind = down_weight.dtype
    block = rows * chunk * kind.itemsize
    scratch_bytes = (STAGES + 1) * n_tp * block + chunks * (2 * n_ep + n_tp) * block
    saved = pl.pallas_call(
        functools.partial(kernel, n_ep, n_tp, n_dp, chunk),
        out_shape=pltpu.VMEM((1, 1, rows, n_tp * hidden), kind),
        in_specs=[pl.BlockSpec(memory_space=pl.ANY), pl.BlockSpec(memory_space=pltpu.SMEM)],
        out_specs=pl.BlockSpec(memory_space=pltpu.VMEM),
        scratch_shapes=[
            pltpu.VMEM((STAGES, chunk, width), kind),
            pltpu.VMEM((width, chunk), kind),
            pltpu.VMEM((chunks, n_ep, rows, chunk), kind),
            pltpu.VMEM((chunks, n_tp, rows, chunk), kind),
            pltpu.SemaphoreType.DMA((STAGES,)),
            pltpu.SemaphoreType.DMA((chunks, n_ep)),
            pltpu.SemaphoreType.DMA((chunks, n_ep)),
            pltpu.SemaphoreType.DMA((chunks, n_tp)),
            pltpu.SemaphoreType.DMA((chunks, n_tp)),
            pltpu.SemaphoreType.DMA((chunks,)),
        ] + [pltpu.VMEM((n_ep, rows, chunk), kind) for _ in range(chunks)],
        compiler_params=pltpu.CompilerParams(
            collective_id=0, has_side_effects=True, vmem_limit_bytes=scratch_bytes + SPARE),
    )(down_weight, jnp.transpose(owned_span, (0, 2, 1)))
    return write_out(saved)


def solution(mesh):
    return jax.shard_map(
        local,
        mesh=mesh,
        in_specs=(P("ep", "tp", "dp"), P()),
        out_specs=P("ep", "tp", "dp", None),
        check_vma=False,
    )
```

```python
import functools

import jax
import jax.numpy as jnp
from jax import lax
from jax.experimental import pallas as pl
from jax.experimental.pallas import tpu as pltpu
from jax.sharding import PartitionSpec as P

MESH = pl.DeviceIdType.MESH
LANES = 128
SUBLANES = 16
CHUNK = 256
STAGES = 4
AHEAD = 2
SPARE = 3 << 20
WRITES = 8


def pick(values, index):
    chosen = values[0]
    for b in range(1, len(values)):
        chosen = jnp.where(index == b, values[b], chosen)
    return chosen


def kernel(n_ep, n_tp, n_dp, chunk, weight, span, out, stage, turned, send, relay,
           load_sem, ep_send, ep_recv, tp_send, tp_recv, own_sem, early, middle, spread, late,
           early_send, early_recv, fan_send, fan_recv, late_sem, *arrived):
    my_ep = lax.axis_index("ep")
    my_tp = lax.axis_index("tp")
    my_dp = lax.axis_index("dp")
    hidden, width = weight.shape[1], weight.shape[2]
    rows = width // n_tp
    chunks = hidden // chunk
    per_expert = n_tp * n_dp

    def load(c):
        return pltpu.make_async_copy(
            weight.at[0, pl.ds(c * chunk, chunk)], stage.at[c % STAGES], load_sem.at[c % STAGES])

    def to_ep(c, d):
        return pltpu.make_async_remote_copy(
            send.at[c, d], arrived[c - 1].at[d], ep_send.at[c, d], ep_recv.at[c, d],
            device_id={"ep": lax.rem(my_ep + d, n_ep)}, device_id_type=MESH)

    def columns(tp, c):
        return out.at[0, 0, :, pl.ds(pl.multiple_of(tp * hidden + c * chunk, chunk), chunk)]

    def to_tp(c, d):
        return pltpu.make_async_remote_copy(
            relay.at[c, d], columns(my_tp, c), tp_send.at[c, d], tp_recv.at[c, d],
            device_id={"tp": lax.rem(my_tp + d, n_tp)}, device_id_type=MESH)

    def from_tp(c, d):
        return pltpu.make_async_remote_copy(
            relay.at[c, d], columns(lax.rem(my_tp + n_tp - d, n_tp), c), tp_send.at[c, d], tp_recv.at[c, d],
            device_id={"tp": lax.rem(my_tp + d, n_tp)}, device_id_type=MESH)

    def own(c):
        return pltpu.make_async_copy(relay.at[c, 0], columns(my_tp, c), own_sem.at[c])

    def early_to_tp(d):
        return pltpu.make_async_remote_copy(
            early.at[d - 1], middle.at[d], early_send.at[d], early_recv.at[d],
            device_id={"tp": lax.rem(my_tp + d, n_tp)}, device_id_type=MESH)

    def fan(d):
        return pltpu.make_async_remote_copy(
            middle, spread.at[d - 1], fan_send.at[d], fan_recv.at[d],
            device_id={"ep": lax.rem(my_ep + d, n_ep)}, device_id_type=MESH)

    def late_own(p):
        return pltpu.make_async_copy(late.at[p], columns(lax.rem(my_tp + n_tp - p, n_tp), 0), late_sem.at[p])

    for c in range(min(STAGES, chunks)):
        load(c).start()

    barrier = pltpu.get_barrier_semaphore()
    for d in range(1, n_ep):
        pl.semaphore_signal(barrier, inc=1, device_id={"ep": lax.rem(my_ep + d, n_ep)}, device_id_type=MESH)
    for d in range(1, n_tp):
        pl.semaphore_signal(barrier, inc=1, device_id={"tp": lax.rem(my_tp + d, n_tp)}, device_id_type=MESH)

    wanted = []
    for d in range(n_ep):
        i = lax.rem(my_ep + d, n_ep)
        total = jnp.int32(0)
        for j in range(n_tp):
            g = span[i, my_dp, j]
            total = total + jnp.where(g // per_expert == my_ep, g % per_expert - my_dp * n_tp, 0)
        wanted.append(total)
    slot = []
    for d in range(n_tp):
        j = lax.rem(my_tp + d, n_tp)
        slot.append(lax.rem(my_ep + n_ep - span[my_ep, my_dp, j] // per_expert, n_ep))

    sooner = []
    for d in range(n_tp):
        j = lax.rem(my_tp + d, n_tp)
        total = jnp.int32(0)
        for i in range(n_ep):
            g = span[i, my_dp, j]
            total = total + jnp.where(g // per_expert == my_ep, g % per_expert - my_dp * n_tp, 0)
        sooner.append(total)

    def turn(c):
        load(c).wait()

        @pl.loop(0, width // LANES)
        def _(b):
            at = pl.multiple_of(b * LANES, LANES)
            turned[pl.ds(at, LANES), :] = stage[c % STAGES, :, pl.ds(at, LANES)].T

        if c + STAGES < chunks:
            load(c + STAGES).start()

    def block_of(index):
        return pick([turned[b * rows:(b + 1) * rows, :] for b in range(n_tp)], index)

    def first_half(c):
        turn(c)
        for d in range(n_ep - 1, -1, -1):
            if d == 0:
                arrived[c - 1][0] = block_of(wanted[d])
            else:
                send[c, d] = block_of(wanted[d])
                to_ep(c, d).start()

    def second_half(c):
        for d in range(1, n_ep):
            to_ep(c, d).wait_recv()
        for d in range(n_tp - 1, -1, -1):
            relay[c, d] = pick([arrived[c - 1][s] for s in range(n_ep)], slot[d])
            if d == 0:
                own(c).start()
            else:
                to_tp(c, d).start()

    turn(0)
    for d in range(1, n_tp):
        early[d - 1] = block_of(sooner[d])
        if d == 1:
            pl.semaphore_wait(barrier, n_ep + n_tp - 2)
        early_to_tp(d).start()
    middle[0] = block_of(sooner[0])

    for step in range(1, chunks + AHEAD):
        if step < chunks:
            first_half(step)
        if step == chunks:
            for d in range(1, n_tp):
                early_to_tp(d).wait_recv()
            for d in range(1, n_ep):
                fan(d).start()
        if step > AHEAD:
            second_half(step - AHEAD)

    for d in range(1, n_ep):
        fan(d).wait_recv()
    for p in range(n_tp):
        late[p] = pick([middle[p]] + [spread[d - 1, p] for d in range(1, n_ep)], slot[0])
        late_own(p).start()

    for d in range(1, n_ep):
        fan(d).wait_send()
    for d in range(1, n_tp):
        early_to_tp(d).wait_send()
    for c in range(1, chunks):
        for d in range(1, n_ep):
            to_ep(c, d).wait_send()
        for d in range(1, n_tp):
            from_tp(c, d).wait_recv()
            to_tp(c, d).wait_send()
        own(c).wait()
    for p in range(n_tp):
        late_own(p).wait()


def writer(saved, out, sem):
    pieces = sem.shape[0]
    rows = saved.shape[2] // pieces
    copies = [
        pltpu.make_async_copy(
            saved.at[0, 0, pl.ds(p * rows, rows)], out.at[0, 0, pl.ds(p * rows, rows)], sem.at[p])
        for p in range(pieces)
    ]
    for copy in copies:
        copy.start()
    for copy in copies:
        copy.wait()


def write_out(saved):
    tiles = max(saved.shape[2] // SUBLANES, 1)
    pieces = max(p for p in range(1, WRITES + 1) if tiles % p == 0)
    return pl.pallas_call(
        writer,
        out_shape=jax.ShapeDtypeStruct(saved.shape, saved.dtype),
        in_specs=[pl.BlockSpec(memory_space=pltpu.VMEM)],
        out_specs=pl.BlockSpec(memory_space=pl.ANY),
        scratch_shapes=[pltpu.SemaphoreType.DMA((pieces,))],
        compiler_params=pltpu.CompilerParams(vmem_limit_bytes=SPARE),
    )(saved)


def local(down_weight, owned_span):
    n_ep, n_tp, n_dp = (lax.axis_size(a) for a in ("ep", "tp", "dp"))
    _, hidden, width = down_weight.shape
    rows = width // n_tp
    chunk = min(CHUNK, hidden)
    chunks = hidden // chunk
    kind = down_weight.dtype
    block = rows * chunk * kind.itemsize
    scratch_bytes = (STAGES + 1) * n_tp * block + chunks * (2 * n_ep + n_tp) * block + (n_ep + 2) * n_tp * block
    saved = pl.pallas_call(
        functools.partial(kernel, n_ep, n_tp, n_dp, chunk),
        out_shape=pltpu.VMEM((1, 1, rows, n_tp * hidden), kind),
        in_specs=[pl.BlockSpec(memory_space=pl.ANY), pl.BlockSpec(memory_space=pltpu.SMEM)],
        out_specs=pl.BlockSpec(memory_space=pltpu.VMEM),
        scratch_shapes=[
            pltpu.VMEM((STAGES, chunk, width), kind),
            pltpu.VMEM((width, chunk), kind),
            pltpu.VMEM((chunks, n_ep, rows, chunk), kind),
            pltpu.VMEM((chunks, n_tp, rows, chunk), kind),
            pltpu.SemaphoreType.DMA((STAGES,)),
            pltpu.SemaphoreType.DMA((chunks, n_ep)),
            pltpu.SemaphoreType.DMA((chunks, n_ep)),
            pltpu.SemaphoreType.DMA((chunks, n_tp)),
            pltpu.SemaphoreType.DMA((chunks, n_tp)),
            pltpu.SemaphoreType.DMA((chunks,)),
                    pltpu.VMEM((n_tp - 1, rows, chunk), kind),
            pltpu.VMEM((n_tp, rows, chunk), kind),
            pltpu.VMEM((n_ep - 1, n_tp, rows, chunk), kind),
            pltpu.VMEM((n_tp, rows, chunk), kind),
            pltpu.SemaphoreType.DMA((n_tp,)),
            pltpu.SemaphoreType.DMA((n_tp,)),
            pltpu.SemaphoreType.DMA((n_ep,)),
            pltpu.SemaphoreType.DMA((n_ep,)),
            pltpu.SemaphoreType.DMA((n_tp,)),
        ] + [pltpu.VMEM((n_ep, rows, chunk), kind) for _ in range(chunks - 1)],
        compiler_params=pltpu.CompilerParams(
            collective_id=0, has_side_effects=True, vmem_limit_bytes=scratch_bytes + SPARE),
    )(down_weight, jnp.transpose(owned_span, (0, 2, 1)))
    return write_out(saved)


def solution(mesh):
    return jax.shard_map(
        local,
        mesh=mesh,
        in_specs=(P("ep", "tp", "dp"), P()),
        out_specs=P("ep", "tp", "dp", None),
        check_vma=False,
    )
```

```python
import functools

import jax
import jax.numpy as jnp
from jax import lax
from jax.experimental import pallas as pl
from jax.experimental.pallas import tpu as pltpu
from jax.sharding import PartitionSpec as P

MESH = pl.DeviceIdType.MESH
LANES = 128
SUBLANES = 16
CHUNK = 256
STAGES = 4
AHEAD = 2
SPARE = 3 << 20
WRITES = 8


def pick(values, index):
    chosen = values[0]
    for b in range(1, len(values)):
        chosen = jnp.where(index == b, values[b], chosen)
    return chosen


def kernel(n_ep, n_tp, n_dp, chunk, weight, span, out, stage, turned, send, relay,
           load_sem, ep_send, ep_recv, tp_send, tp_recv, own_sem, early, middle, spread, late,
           early_send, early_recv, fan_send, fan_recv, late_sem, *arrived):
    my_ep = lax.axis_index("ep")
    my_tp = lax.axis_index("tp")
    my_dp = lax.axis_index("dp")
    hidden, width = weight.shape[1], weight.shape[2]
    rows = width // n_tp
    chunks = hidden // chunk
    per_expert = n_tp * n_dp

    def load(c):
        return pltpu.make_async_copy(
            weight.at[0, pl.ds(c * chunk, chunk)], stage.at[c % STAGES], load_sem.at[c % STAGES])

    def to_ep(c, d):
        return pltpu.make_async_remote_copy(
            send.at[c, d], arrived[c - 1].at[d], ep_send.at[c, d], ep_recv.at[c, d],
            device_id={"ep": lax.rem(my_ep + d, n_ep)}, device_id_type=MESH)

    def columns(tp, c):
        return out.at[0, 0, :, pl.ds(pl.multiple_of(tp * hidden + c * chunk, chunk), chunk)]

    def to_tp(c, d):
        return pltpu.make_async_remote_copy(
            relay.at[c, d], columns(my_tp, c), tp_send.at[c, d], tp_recv.at[c, d],
            device_id={"tp": lax.rem(my_tp + d, n_tp)}, device_id_type=MESH)

    def from_tp(c, d):
        return pltpu.make_async_remote_copy(
            relay.at[c, d], columns(lax.rem(my_tp + n_tp - d, n_tp), c), tp_send.at[c, d], tp_recv.at[c, d],
            device_id={"tp": lax.rem(my_tp + d, n_tp)}, device_id_type=MESH)

    def own(c):
        return pltpu.make_async_copy(relay.at[c, 0], columns(my_tp, c), own_sem.at[c])

    def early_to_tp(d):
        return pltpu.make_async_remote_copy(
            early.at[d - 1], middle.at[d], early_send.at[d], early_recv.at[d],
            device_id={"tp": lax.rem(my_tp + d, n_tp)}, device_id_type=MESH)

    def fan(d):
        return pltpu.make_async_remote_copy(
            middle, spread.at[d - 1], fan_send.at[d], fan_recv.at[d],
            device_id={"ep": lax.rem(my_ep + d, n_ep)}, device_id_type=MESH)

    def late_own(p):
        return pltpu.make_async_copy(late.at[p], columns(lax.rem(my_tp + n_tp - p, n_tp), 0), late_sem.at[p])

    load(0).start()

    barrier = pltpu.get_barrier_semaphore()
    for d in range(1, n_ep):
        pl.semaphore_signal(barrier, inc=1, device_id={"ep": lax.rem(my_ep + d, n_ep)}, device_id_type=MESH)
    for d in range(1, n_tp):
        pl.semaphore_signal(barrier, inc=1, device_id={"tp": lax.rem(my_tp + d, n_tp)}, device_id_type=MESH)

    wanted = []
    for d in range(n_ep):
        i = lax.rem(my_ep + d, n_ep)
        total = jnp.int32(0)
        for j in range(n_tp):
            g = span[i, my_dp, j]
            total = total + jnp.where(g // per_expert == my_ep, g % per_expert - my_dp * n_tp, 0)
        wanted.append(total)
    slot = []
    for d in range(n_tp):
        j = lax.rem(my_tp + d, n_tp)
        slot.append(lax.rem(my_ep + n_ep - span[my_ep, my_dp, j] // per_expert, n_ep))

    sooner = []
    for d in range(n_tp):
        j = lax.rem(my_tp + d, n_tp)
        total = jnp.int32(0)
        for i in range(n_ep):
            g = span[i, my_dp, j]
            total = total + jnp.where(g // per_expert == my_ep, g % per_expert - my_dp * n_tp, 0)
        sooner.append(total)

    def turn(c):
        load(c).wait()
        if c == 0:
            for later in range(1, min(STAGES, chunks)):
                load(later).start()

        @pl.loop(0, width // LANES)
        def _(b):
            at = pl.multiple_of(b * LANES, LANES)
            turned[pl.ds(at, LANES), :] = stage[c % STAGES, :, pl.ds(at, LANES)].T

        if c + STAGES < chunks:
            load(c + STAGES).start()

    def block_of(index):
        return pick([turned[b * rows:(b + 1) * rows, :] for b in range(n_tp)], index)

    def first_half(c):
        turn(c)
        for d in range(n_ep - 1, -1, -1):
            if d == 0:
                arrived[c - 1][0] = block_of(wanted[d])
            else:
                send[c, d] = block_of(wanted[d])
                to_ep(c, d).start()

    def second_half(c):
        for d in range(1, n_ep):
            to_ep(c, d).wait_recv()
        for k in range(1, n_tp):
            d = jnp.where(my_tp < n_tp // 2, k, n_tp - k)
            index = jnp.where(my_tp < n_tp // 2, slot[k], slot[n_tp - k])
            relay[c, d] = pick([arrived[c - 1][s] for s in range(n_ep)], index)
            to_tp(c, d).start()
        relay[c, 0] = pick([arrived[c - 1][s] for s in range(n_ep)], slot[0])
        own(c).start()

    turn(0)
    for d in range(1, n_tp):
        early[d - 1] = block_of(sooner[d])
        if d == 1:
            pl.semaphore_wait(barrier, n_ep + n_tp - 2)
        early_to_tp(d).start()
    middle[0] = block_of(sooner[0])

    for step in range(1, chunks + AHEAD):
        if step < chunks:
            first_half(step)
        if step == chunks:
            for d in range(1, n_tp):
                early_to_tp(d).wait_recv()
            for d in range(1, n_ep):
                fan(d).start()
        if step > AHEAD:
            second_half(step - AHEAD)

    for d in range(1, n_ep):
        fan(d).wait_recv()
    for p in range(n_tp):
        late[p] = pick([middle[p]] + [spread[d - 1, p] for d in range(1, n_ep)], slot[0])
        late_own(p).start()

    for d in range(1, n_ep):
        fan(d).wait_send()
    for d in range(1, n_tp):
        early_to_tp(d).wait_send()
    for c in range(1, chunks):
        for d in range(1, n_ep):
            to_ep(c, d).wait_send()
        for d in range(1, n_tp):
            from_tp(c, d).wait_recv()
            to_tp(c, d).wait_send()
        own(c).wait()
    for p in range(n_tp):
        late_own(p).wait()


def writer(saved, out, sem):
    pieces = sem.shape[0]
    rows = saved.shape[2] // pieces
    copies = [
        pltpu.make_async_copy(
            saved.at[0, 0, pl.ds(p * rows, rows)], out.at[0, 0, pl.ds(p * rows, rows)], sem.at[p])
        for p in range(pieces)
    ]
    for copy in copies:
        copy.start()
    for copy in copies:
        copy.wait()


def write_out(saved):
    tiles = max(saved.shape[2] // SUBLANES, 1)
    pieces = max(p for p in range(1, WRITES + 1) if tiles % p == 0)
    return pl.pallas_call(
        writer,
        out_shape=jax.ShapeDtypeStruct(saved.shape, saved.dtype),
        in_specs=[pl.BlockSpec(memory_space=pltpu.VMEM)],
        out_specs=pl.BlockSpec(memory_space=pl.ANY),
        scratch_shapes=[pltpu.SemaphoreType.DMA((pieces,))],
        compiler_params=pltpu.CompilerParams(vmem_limit_bytes=SPARE),
    )(saved)


def local(down_weight, owned_span):
    n_ep, n_tp, n_dp = (lax.axis_size(a) for a in ("ep", "tp", "dp"))
    _, hidden, width = down_weight.shape
    rows = width // n_tp
    chunk = min(CHUNK, hidden)
    chunks = hidden // chunk
    kind = down_weight.dtype
    block = rows * chunk * kind.itemsize
    scratch_bytes = (STAGES + 1) * n_tp * block + chunks * (2 * n_ep + n_tp) * block + (n_ep + 2) * n_tp * block
    saved = pl.pallas_call(
        functools.partial(kernel, n_ep, n_tp, n_dp, chunk),
        out_shape=pltpu.VMEM((1, 1, rows, n_tp * hidden), kind),
        in_specs=[pl.BlockSpec(memory_space=pl.ANY), pl.BlockSpec(memory_space=pltpu.SMEM)],
        out_specs=pl.BlockSpec(memory_space=pltpu.VMEM),
        scratch_shapes=[
            pltpu.VMEM((STAGES, chunk, width), kind),
            pltpu.VMEM((width, chunk), kind),
            pltpu.VMEM((chunks, n_ep, rows, chunk), kind),
            pltpu.VMEM((chunks, n_tp, rows, chunk), kind),
            pltpu.SemaphoreType.DMA((STAGES,)),
            pltpu.SemaphoreType.DMA((chunks, n_ep)),
            pltpu.SemaphoreType.DMA((chunks, n_ep)),
            pltpu.SemaphoreType.DMA((chunks, n_tp)),
            pltpu.SemaphoreType.DMA((chunks, n_tp)),
            pltpu.SemaphoreType.DMA((chunks,)),
                    pltpu.VMEM((n_tp - 1, rows, chunk), kind),
            pltpu.VMEM((n_tp, rows, chunk), kind),
            pltpu.VMEM((n_ep - 1, n_tp, rows, chunk), kind),
            pltpu.VMEM((n_tp, rows, chunk), kind),
            pltpu.SemaphoreType.DMA((n_tp,)),
            pltpu.SemaphoreType.DMA((n_tp,)),
            pltpu.SemaphoreType.DMA((n_ep,)),
            pltpu.SemaphoreType.DMA((n_ep,)),
            pltpu.SemaphoreType.DMA((n_tp,)),
        ] + [pltpu.VMEM((n_ep, rows, chunk), kind) for _ in range(chunks - 1)],
        compiler_params=pltpu.CompilerParams(
            collective_id=0, has_side_effects=True, vmem_limit_bytes=scratch_bytes + SPARE),
    )(down_weight, jnp.transpose(owned_span, (0, 2, 1)))
    return write_out(saved)


def solution(mesh):
    return jax.shard_map(
        local,
        mesh=mesh,
        in_specs=(P("ep", "tp", "dp"), P()),
        out_specs=P("ep", "tp", "dp", None),
        check_vma=False,
    )
```
